32 devices in a mesh: dp: 8 (over z, x), mp: 4 (over y, core).
Axes of the slice: x: 2, y: 2, z: 4, core: 2. Of those that a mesh axis runs over, the one named last changes fastest.
Arguments:
- hidden_in: bfloat16 [8192, 2048], P('dp', 'mp'), may hold values from -6 to 6
- token_ids: int32 [8192], P('dp'), may hold values from 0 to 128001, as said below
- passage_counts: int32 [16], P('dp'), may hold values from 1 to 4, as said below
- positive_doc: int32 [1024], P('dp'), may hold values from 0 to 15
- queries: bfloat16 [1024, 2048], P('dp', 'mp'), may hold values from -6 to 6
- norm_gain: float32 [2048], replicated, may hold values from 0.5 to 1.5
- w_gate: bfloat16 [2048, 7168], P(None, 'mp'), may hold values from -0.125 to 0.125
- w_up: bfloat16 [2048, 7168], P(None, 'mp'), may hold values from -0.125 to 0.125
- w_down: bfloat16 [7168, 2048], P('mp'), may hold values from -0.0625 to 0.0625
Outputs:
- query_loss: float32 [1024], P('dp')
- hidden_grad: bfloat16 [8192, 2048], P('dp', 'mp')
The draws below stay inside these ranges and needn't reach their ends.
Inputs may be any that keep to these rules, and one draw needn't show every extreme that they name: `passage_counts`: A document has 1 to 4 passages; every draw has a dp index whose documents all have 4. The live passages hold 40 passages in all. `token_ids`: 128001 marks padding; it stands only at the tail of a document's last live passage, and every live passage has a token that is not padding.
All inputs are finite; a program needn't handle non-finite values.
Results may differ from the reference program's by a relative error of at most 0.023.
Values may be sent and summed in bfloat16 or wider, within the bound.
A program may use at most 128 MiB of HBM per device.

```python
import jax
import jax.numpy as jnp
from jax import lax

D = 2048
FF = 7168
L = 128
PMAX = 4
DOC_DEV = 2
CAP = 20
DOCS = 16
PASSAGES = 64
QUERIES = 1024
ROWS = 8192
N_DP = 8


pad_token = 128001


def make_counts(key):
    half = DOCS // 2
    order = jax.random.permutation(jax.random.fold_in(key, 101), half)
    base = 1 + order % PMAX
    heavy = jax.random.randint(jax.random.fold_in(key, 102), (), 0, half // DOC_DEV)
    base = jnp.where(jnp.arange(half) // DOC_DEV == heavy, PMAX, base)
    return jnp.concatenate([base, PMAX + 1 - base]).astype(jnp.int32)


def draw_passage_counts(key, part):
    return make_counts(key)


def draw_token_ids(key, part):
    counts = make_counts(key)
    passage_total = DOCS * PMAX
    passage_index = jnp.arange(passage_total, dtype=jnp.int32)
    last_live = passage_index % PMAX == jnp.repeat(counts, PMAX) - 1
    length = jax.random.randint(jax.random.fold_in(key, 106), (passage_total,), 1, L + 1)
    length = jnp.where(last_live, length, L)
    position = jnp.arange(L, dtype=jnp.int32)
    words = jax.random.randint(jax.random.fold_in(key, 107), (passage_total, L), 0, 128000)
    tokens = jnp.where(position[None, :] < length[:, None], words, pad_token)
    return tokens.reshape(passage_total * L).astype(jnp.int32)


def touch_ends(drawn, key, least, largest):
    place = [jax.random.randint(jax.random.fold_in(key, axis), (), 0, length) for axis, length in enumerate(drawn.shape)]
    widest = drawn.shape.index(max(drawn.shape))
    next_to = place[:widest] + [(place[widest] + 1) % drawn.shape[widest]] + place[widest + 1:]
    return drawn.at[tuple(place)].set(least).at[tuple(next_to)].set(largest)


def levels(own_key, extent, pieces, low, largest):
    def one(dim, shards_of):
        draws = jax.random.uniform(jax.random.fold_in(jax.random.fold_in(own_key, 6), dim), (shards_of,), jnp.float32, low / len(pieces), largest / len(pieces))
        return jnp.repeat(jnp.exp(draws), extent[dim] // shards_of).reshape((-1,) + (1,) * (len(extent) - dim - 1))

    level = one(*pieces[0])
    for cut in pieces[1:]:
        level = level * one(*cut)
    return level


def scatter_about(rng, dims, deviation, reach, cuts=(), kind=jnp.bfloat16):
    drawn = jax.random.normal(rng, dims, jnp.float32) * deviation
    if len(cuts) > 0:
        drawn = levels(rng, dims, cuts, -0.22, 0.18) * drawn
    return jnp.clip(drawn, min=-reach, max=reach).astype(kind)


def setup_inputs(seed: int = 0) -> dict:
    key_of = jax.random.split(jax.random.key(seed), 10)
    return {
        "hidden_in": scatter_about(key_of[0], (ROWS, D), 1.0, 6.0, ((0, 8), (1, 4))),
        "token_ids": draw_token_ids(jax.random.fold_in(key_of[9], 71), 0),
        "passage_counts": draw_passage_counts(jax.random.fold_in(key_of[9], 71), 0),
        "positive_doc": touch_ends(jax.random.randint(key_of[3], (QUERIES,), 0, DOCS), jax.random.fold_in(key_of[3], 1), 0, DOCS - 1).astype(jnp.int32),
        "queries": scatter_about(key_of[4], (QUERIES, D), 1.0, 6.0, ((0, 8), (1, 4))),
        "norm_gain": jnp.clip(1.0 + 0.1 * jax.random.normal(key_of[5], (D,), jnp.float32), 0.5, 1.5),
        "w_gate": scatter_about(key_of[6], (D, FF), D ** -0.5, 0.125, ((1, 4),)),
        "w_up": scatter_about(key_of[7], (D, FF), D ** -0.5, 0.125, ((1, 4),)),
        "w_down": scatter_about(key_of[8], (FF, D), FF ** -0.5, 0.0625, ((0, 4),)),
    }


pad_token = 128001
score_scale = 20.0
loss_seed = 4096.0
norm_epsilon = 1e-05
unit_epsilon = 1e-06

def layer_forward(rows, norm_gain, w_gate, w_up, w_down):
    row_float = rows.astype(jnp.float32)
    rms_scale = lax.rsqrt(lax.optimization_barrier(jnp.mean(row_float * row_float, axis=1, keepdims=True)) + norm_epsilon)
    normed = (row_float * rms_scale * norm_gain[None, :]).astype(jnp.bfloat16)
    gate = jnp.dot(normed, w_gate, preferred_element_type=jnp.float32)
    up = jnp.dot(normed, w_up, preferred_element_type=jnp.float32)
    sigmoid_gate = jax.nn.sigmoid(gate)
    hidden = (gate * sigmoid_gate * up).astype(jnp.bfloat16)
    branch = jnp.dot(hidden, w_down, preferred_element_type=jnp.float32)
    return (row_float, rms_scale, gate, up, sigmoid_gate, branch)

def reference(hidden_in, token_ids, passage_counts, positive_doc, queries, norm_gain, w_gate, w_up, w_down):
    block_len = L // 4
    block_total = DOCS * PMAX * 4
    block_index = jnp.arange(block_total, dtype=jnp.int32)
    live_block = block_index // 4 % PMAX < jnp.repeat(passage_counts, PMAX * 4)
    token_live = (token_ids.reshape(block_total, block_len) != pad_token) & live_block[:, None]
    chosen = jnp.nonzero(live_block, size=N_DP * CAP)[0].astype(jnp.int32)
    task_rows = hidden_in.reshape(block_total, block_len, D)[chosen].reshape(N_DP, CAP * block_len, D)
    task_row_mask = token_live[chosen].astype(jnp.float32).reshape(N_DP, CAP, block_len)

    def pool_group(pair):
        rows, mask = pair
        row_float, rms_scale, gate, up, sigmoid_gate, branch = layer_forward(rows, norm_gain, w_gate, w_up, w_down)
        output = (row_float + branch).reshape(CAP, block_len, D)
        return lax.optimization_barrier(jnp.sum(output * mask[:, :, None], axis=1))
    pooled = lax.map(pool_group, (task_rows, task_row_mask)).reshape(N_DP * CAP, D)
    block_sums = jnp.zeros((block_total, D), jnp.float32).at[chosen].set(pooled)
    passage_sum = block_sums.reshape(PASSAGES, 4, D).sum(axis=1)
    token_total = lax.optimization_barrier(jnp.sum(token_live.reshape(PASSAGES, L).astype(jnp.float32), axis=1))
    divisor = jnp.maximum(token_total, 1.0)
    passage_vec = (passage_sum / divisor[:, None]).astype(jnp.bfloat16)
    passage_live = live_block.reshape(PASSAGES, 4)[:, 0].astype(jnp.float32)
    vec_float = passage_vec.astype(jnp.float32)
    query_float = queries.astype(jnp.float32)
    raw_score = lax.dot_general(queries, passage_vec, (((1,), (1,)), ((), ())), preferred_element_type=jnp.float32)
    query_scale = lax.rsqrt(lax.optimization_barrier(jnp.sum(query_float * query_float, axis=1)) + unit_epsilon)
    passage_scale = lax.rsqrt(lax.optimization_barrier(jnp.sum(vec_float * vec_float, axis=1)) + unit_epsilon)
    scores = score_scale * raw_score * query_scale[:, None] * passage_scale[None, :]
    weights = passage_live[None, :] * jnp.exp(scores)
    doc_mass = weights.reshape(QUERIES, DOCS, PMAX).sum(axis=2)
    total_mass = doc_mass.sum(axis=1)
    positive_hit = (positive_doc[:, None] == jnp.arange(DOCS, dtype=jnp.int32)[None, :]).astype(jnp.float32)
    positive_mass = lax.optimization_barrier(jnp.sum(doc_mass * positive_hit, axis=1))
    query_loss = jnp.log(total_mass) - jnp.log(positive_mass)
    positive_pass = jnp.repeat(positive_hit, PMAX, axis=1)
    coefficient = loss_seed * score_scale * query_scale[:, None] * (weights / total_mass[:, None] - positive_pass * weights / positive_mass[:, None])
    weighted_queries = lax.dot_general(coefficient.astype(jnp.bfloat16), queries, (((0,), (0,)), ((), ())), preferred_element_type=jnp.float32)
    norm_term = lax.optimization_barrier(jnp.sum(coefficient * raw_score, axis=0))
    vec_change = passage_scale[:, None] * weighted_queries - vec_float * (passage_scale ** 3 * norm_term)[:, None]
    token_grad = (vec_change / divisor[:, None]).astype(jnp.bfloat16)
    block_grad = jnp.repeat(token_grad, 4, axis=0)[chosen].reshape(N_DP, CAP, D)

    def grad_group(triple):
        rows, mask, grad = triple
        row_float, rms_scale, gate, up, sigmoid_gate, branch = layer_forward(rows, norm_gain, w_gate, w_up, w_down)
        out_float = (mask[:, :, None] * grad[:, None, :].astype(jnp.float32)).reshape(CAP * block_len, D)
        out_grad = out_float.astype(jnp.bfloat16)
        hidden_grad = lax.dot_general(out_grad, w_down, (((1,), (1,)), ((), ())), preferred_element_type=jnp.float32)
        gate_grad = (hidden_grad * up * sigmoid_gate * (1.0 + gate * (1.0 - sigmoid_gate))).astype(jnp.bfloat16)
        up_grad = (hidden_grad * gate * sigmoid_gate).astype(jnp.bfloat16)
        normed_grad = lax.dot_general(gate_grad, w_gate, (((1,), (1,)), ((), ())), preferred_element_type=jnp.float32)
        normed_grad = normed_grad + lax.dot_general(up_grad, w_up, (((1,), (1,)), ((), ())), preferred_element_type=jnp.float32)
        inner = lax.optimization_barrier(jnp.mean(row_float * norm_gain[None, :] * normed_grad, axis=1))
        input_grad = out_float + rms_scale * norm_gain[None, :] * normed_grad - row_float * rms_scale ** 3 * inner[:, None]
        return input_grad.astype(jnp.bfloat16).reshape(CAP, block_len * D)
    task_grads = lax.map(grad_group, (task_rows, task_row_mask, block_grad)).reshape(N_DP * CAP, block_len * D)
    grad_rows = jnp.zeros((block_total, block_len * D), jnp.bfloat16).at[chosen].set(task_grads)
    return (query_loss, grad_rows.reshape(ROWS, D))
```

```python
import functools

import jax
import jax.numpy as jnp
from jax import lax
from jax.experimental import pallas as pl
from jax.experimental.pallas import tpu as pltpu
from jax.sharding import PartitionSpec as P

L = 128

pad_token = 128001
score_scale = 20.0
loss_seed = 4096.0
norm_epsilon = 1e-05
unit_epsilon = 1e-06
lane = 128
chunk_pass = 2
MESH = pl.DeviceIdType.MESH
f32 = jnp.float32
bf16 = jnp.bfloat16


def dot_nn(left, right):
    return lax.dot_general(left, right, (((1,), (0,)), ((), ())), preferred_element_type=f32)


def dot_nt(left, right):
    return lax.dot_general(left, right, (((1,), (1,)), ((), ())), preferred_element_type=f32)


def tile_of(width):
    return 256 if width % 256 == 0 else lane


def kernel(
    dims,
    hidden, queries, w_gate, w_up, w_down, tokens, counts, positive, gain,
    loss_out, grad_out,
    x_buf, q_buf, wg, wu, wd, a_buf, b_buf, c_buf, normed, act, dgate, dup, rms,
    act_pool, row_pool, branch, everyone, term_send, term_recv, tok_grad, g_row, inner_x,
    mask_row, near_send, near_recv, far_send, far_recv, kept, staged,
    load_sem, out_sem, xn_s, xn_r, xf_s, xf_r, xr_s, xr_r, br_s, br_r, in_s, in_r,
    ev_s, ev_r, tm_s, tm_r, ns_s, ns_r, fs_s, fs_r,
):
    dp, mp, far, rows, width, model, hid, passes, most, chunks, crow = dims
    me = lax.axis_index("mp")
    dme = lax.axis_index("dp")
    chip, core = me // 2, me % 2
    partner = chip * 2 + (1 - core)

    def same(j):
        return ((chip + j + far) % far) * 2 + core

    def other(j):
        return ((chip + j + far) % far) * 2 + (1 - core)

    def chunk_rows(c):
        return pl.ds(pl.multiple_of(c * crow, crow), crow)

    def remote(src, dst, send, recv, d, m):
        return pltpu.make_async_remote_copy(
            src_ref=src, dst_ref=dst, send_sem=send, recv_sem=recv,
            device_id=(d, m), device_id_type=MESH,
        )

    load_x = pltpu.make_async_copy(hidden, x_buf.at[me], load_sem.at[0])
    load_g = pltpu.make_async_copy(w_gate, wg, load_sem.at[1])
    load_u = pltpu.make_async_copy(w_up, wu, load_sem.at[2])
    load_d = pltpu.make_async_copy(w_down, wd, load_sem.at[3])
    load_q = pltpu.make_async_copy(queries, q_buf.at[me], load_sem.at[4])

    barrier = pltpu.get_barrier_semaphore()
    for k in range(1, mp):
        pl.semaphore_signal(barrier, inc=1, device_id=(dme, (me + k) % mp), device_id_type=MESH)
    for k in range(1, dp):
        pl.semaphore_signal(barrier, inc=1, device_id=((dme + k) % dp, me), device_id_type=MESH)
    load_x.start()
    load_g.start()
    load_u.start()
    load_q.start()
    load_d.start()
    pl.semaphore_wait(barrier, mp - 1 + dp - 1)

    def piece(ref, c):
        return ref.at[chunk_rows(c)] if not isinstance(c, int) or c < chunks else ref

    def far_copy(j, c):
        if isinstance(c, int) and c == chunks:
            src, dst = queries, q_buf.at[me]
        else:
            src, dst = hidden.at[chunk_rows(c)], x_buf.at[me, chunk_rows(c)]
        return remote(src, dst, xf_s.at[j - 1, c], xf_r.at[j - 1, c], dme, same(j))

    def near_copy(c):
        if isinstance(c, int) and c == chunks:
            src, dst = queries, q_buf.at[me]
        else:
            src, dst = hidden.at[chunk_rows(c)], x_buf.at[me, chunk_rows(c)]
        return remote(src, dst, xn_s.at[c], xn_r.at[c], dme, partner)

    def relay_copy(j, c):
        if isinstance(c, int) and c == chunks:
            src = dst = q_buf.at[same(-j)]
        else:
            src = dst = x_buf.at[same(-j), chunk_rows(c)]
        return remote(src, dst, xr_s.at[j - 1, c], xr_r.at[j - 1, c], dme, partner)

    def relay(c):
        for j in range(1, far):
            far_copy(j, c).wait_recv()
            relay_copy(j, c).start()

    for c in range(chunks + 1):
        for j in range(1, far):
            far_copy(j, c).start()
        near_copy(c).start()

    pass_index = lax.broadcasted_iota(jnp.int32, (passes, L), 0)
    count = jnp.zeros((passes, L), jnp.int32)
    for d in range(passes // most):
        count = jnp.where(pass_index // most == d, counts[d], count)
    live = (pass_index % most < count).astype(f32)
    mask = jnp.where(tokens[...] != pad_token, live, 0.0)
    mask_row[...] = mask
    divisor = jnp.maximum(jnp.sum(mask, axis=1, keepdims=True), 1.0)
    act_pool[...] = jnp.zeros_like(act_pool)
    row_pool[...] = jnp.zeros_like(row_pool)
    pool_index = lax.broadcasted_iota(jnp.int32, (2 * passes, L), 0)

    tile = tile_of(hid)
    relay(0)
    load_x.wait()
    load_g.wait()
    load_u.wait()

    def forward(c, carry):
        at = chunk_rows(c)
        near_copy(c).wait_recv()
        for j in range(1, far):
            relay_copy(j, c).wait_recv()
        squares = jnp.zeros((crow, 1), f32)
        select = jnp.concatenate(
            [
                jnp.where(pool_index == c * chunk_pass + i, mask_row[pl.ds(c * chunk_pass + i, 1), :], 0.0)
                for i in range(chunk_pass)
            ],
            axis=1,
        ).astype(bf16)
        for m in range(mp):
            piece_x = x_buf[m, at, :].astype(f32)
            squares = squares + jnp.sum(piece_x * piece_x, axis=1, keepdims=True)
        scale = lax.rsqrt(squares / model + norm_epsilon)
        rms[at, :] = scale
        for m in range(mp):
            cols = slice(m * width, (m + 1) * width)
            raw_x = x_buf[m, at, :]
            normed[:, cols] = (raw_x.astype(f32) * scale * gain[:, cols]).astype(bf16)
            row_pool[:, cols] += dot_nn(select, raw_x)
        for t in range(hid // tile):
            cols = slice(t * tile, (t + 1) * tile)
            gate = dot_nn(normed[...], wg[:, cols])
            up = dot_nn(normed[...], wu[:, cols])
            sig = jax.nn.sigmoid(gate)
            b = gate * sig
            a = up * sig * (1.0 + gate * (1.0 - sig))
            hidden_act = (b * up).astype(bf16)
            a_buf[at, cols] = a.astype(bf16)
            b_buf[at, cols] = b.astype(bf16)
            c_buf[at, cols] = (a * gate + b * up).astype(bf16)
            act_pool[:, cols] += dot_nn(select, hidden_act)
            if t == max(hid // tile - 2, 0):
                @pl.when(c + 1 < chunks)
                def _():
                    relay(c + 1)
        return carry

    lax.fori_loop(0, chunks, forward, 0)
    relay(chunks)

    load_d.wait()
    pooled = act_pool[0:passes, :]
    high = pooled.astype(bf16).astype(f32)
    both = jnp.concatenate([high, pooled - high], axis=0).astype(bf16)
    for m in range(mp):
        cols = slice(m * width, (m + 1) * width)
        part = dot_nn(both, wd[:, cols])
        branch[me, :, cols] = (part[0:passes] + part[passes:]).astype(bf16)

    def branch_copy(k):
        return remote(
            branch.at[me], branch.at[me], br_s.at[k - 1], br_r.at[k - 1], dme, (me + k) % mp
        )

    for k in range(1, mp):
        branch_copy(k).start()

    load_q.wait()
    near_copy(chunks).wait_recv()
    for j in range(1, far):
        relay_copy(j, chunks).wait_recv()
    ones = jnp.ones((2 * passes, width), bf16)
    query_square = jnp.zeros((2 * passes, q_buf.shape[1]), f32)
    for m in range(mp):
        query = q_buf[m].astype(f32)
        square = query * query
        top = square.astype(bf16)
        rest = (square - top.astype(f32)).astype(bf16)
        query_square = query_square + dot_nt(ones, top) + dot_nt(ones, rest)
    query_scale = lax.rsqrt(query_square[0:1, :] + unit_epsilon)

    for k in range(1, mp):
        branch_copy(k).wait_recv()
    total = row_pool[0:passes, :]
    for m in range(mp):
        total = total + branch[m].astype(f32)
    everyone[dme, :, 0:model] = (total / divisor).astype(bf16)
    everyone[dme, :, model:] = live.astype(bf16)

    def every_copy(k):
        return remote(
            everyone.at[dme], everyone.at[dme], ev_s.at[k - 1], ev_r.at[k - 1], (dme + k) % dp, me
        )

    for k in range(1, dp):
        every_copy(k).start()
    for k in range(1, dp):
        every_copy(k).wait_recv()

    slabs = [everyone[d].astype(f32) for d in range(dp)]
    slab = jnp.concatenate(slabs, axis=0)
    vec = slab[:, 0:model]
    all_live = slab[:, model : model + 1]
    vec_half = vec.astype(bf16)
    pass_total = dp * passes
    raw = jnp.zeros((pass_total, q_buf.shape[1]), f32)
    for m in range(mp):
        raw = raw + dot_nt(vec_half[:, m * width : (m + 1) * width], q_buf[m])
    pass_scale = lax.rsqrt(jnp.sum(vec * vec, axis=1, keepdims=True) + unit_epsilon)
    weights = all_live * jnp.exp(score_scale * raw * query_scale * pass_scale)
    doc_index = lax.broadcasted_iota(jnp.int32, weights.shape, 0) // most
    hit = (doc_index == positive[...]).astype(f32)
    mass = jnp.sum(weights, axis=0, keepdims=True)
    hit_mass = jnp.sum(weights * hit, axis=0, keepdims=True)
    loss_out[...] = jnp.log(mass) - jnp.log(hit_mass)
    coef = loss_seed * score_scale * query_scale * (weights / mass - hit * weights / hit_mass)
    norm_term = jnp.sum(coef * raw, axis=1, keepdims=True)
    coef_half = coef.astype(bf16)
    for m in range(mp):
        part = dot_nn(coef_half, q_buf[m])
        for d in range(dp):
            term_send[d, :, m * width : (m + 1) * width] = part[d * passes : (d + 1) * passes].astype(bf16)
    wide = jnp.broadcast_to(norm_term, (pass_total, lane))
    for d in range(dp):
        term_send[d, :, model:] = wide[d * passes : (d + 1) * passes].astype(bf16)

    def term_copy(k):
        to = (dme + k) % dp
        return remote(
            term_send.at[to], term_recv.at[dme], tm_s.at[k - 1], tm_r.at[k - 1], to, me
        )

    for k in range(1, dp):
        term_copy(k).start()
    term_recv[dme] = term_send[dme]
    for k in range(1, dp):
        term_copy(k).wait_recv()
    terms = term_recv[0].astype(f32)
    for d in range(1, dp):
        terms = terms + term_recv[d].astype(f32)
    own_vec = everyone[dme].astype(f32)[:, 0:model]
    own_scale = lax.rsqrt(jnp.sum(own_vec * own_vec, axis=1, keepdims=True) + unit_epsilon)
    change = own_scale * terms[:, 0:model] - own_vec * (
        own_scale * own_scale * own_scale * terms[:, model : model + 1]
    )
    token = (change / divisor).astype(bf16).astype(f32)
    tok_grad[...] = token
    token_half = jnp.concatenate([token, jnp.zeros_like(token)], axis=0).astype(bf16)
    for t in range(hid // tile):
        cols = slice(t * tile, (t + 1) * tile)
        g_row[:, cols] = dot_nt(token_half, wd[cols, :])

    def near_part(j, c):
        return remote(
            near_send.at[c, j], near_recv.at[c, j], ns_s.at[c, j], ns_r.at[c, j], dme, partner
        )

    def far_part(j, c):
        return remote(
            far_send.at[c, j - 1], far_recv.at[c, j - 1], fs_s.at[c, j - 1], fs_r.at[c, j - 1], dme, same(j)
        )

    def backward(c, carry):
        at = chunk_rows(c)
        for i in range(chunk_pass):
            row = g_row[pl.ds(c * chunk_pass + i, 1), :]
            spread = jnp.broadcast_to(row, (L, hid)).astype(bf16)
            here = pl.ds(pl.multiple_of(c * crow + i * L, L), L)
            dgate[i * L : (i + 1) * L, :] = a_buf[here, :] * spread
            dup[i * L : (i + 1) * L, :] = b_buf[here, :] * spread

        def partial(block):
            at_rows = pl.ds(pl.multiple_of(block * width, width), width)
            return dot_nt(dgate[...], wg[at_rows, :]) + dot_nt(dup[...], wu[at_rows, :])

        for j in range(1, far):
            near_send[c, j] = partial(other(j)).astype(bf16)
            near_part(j, c).start()
        for j in range(1, far):
            mine = partial(same(j))
            near_part(j, c).wait_recv()
            far_send[c, j - 1] = (mine + near_recv[c, j].astype(f32)).astype(bf16)
            far_part(j, c).start()
        near_send[c, 0] = partial(other(0)).astype(bf16)
        near_part(0, c).start()
        kept[c] = partial(me)
        return carry

    lax.fori_loop(0, chunks, backward, 0)

    g_half = g_row[...].astype(bf16)
    diagonal = jnp.zeros((2 * passes, L), f32)
    for c in range(chunks):
        found = dot_nt(g_half, c_buf[c * crow : (c + 1) * crow, :])
        for i in range(chunk_pass):
            diagonal = diagonal + jnp.where(
                pool_index == c * chunk_pass + i, found[:, i * L : (i + 1) * L], 0.0
            )
    inner_x[me] = diagonal[0:passes]

    def inner_copy(k):
        return remote(
            inner_x.at[me], inner_x.at[me], in_s.at[k - 1], in_r.at[k - 1], dme, (me + k) % mp
        )

    for k in range(1, mp):
        inner_copy(k).start()
    for k in range(1, mp):
        inner_copy(k).wait_recv()
    inner = inner_x[0]
    for m in range(1, mp):
        inner = inner + inner_x[m]
    inner_col = jnp.transpose(inner / model)
    mask_col = jnp.transpose(mask_row[...])
    own = pl.ds(pl.multiple_of(me * width, width), width)
    own_gain = gain[:, own]
    for c in range(chunks):
        near_part(0, c).wait_recv()
        for j in range(1, far):
            far_part(j, c).wait_recv()
        for i in range(chunk_pass):
            p = c * chunk_pass + i
            piece_rows = slice(i * L, (i + 1) * L)
            summed = kept[c, piece_rows, :] + near_recv[c, 0, piece_rows, :].astype(f32)
            for j in range(1, far):
                summed = summed + far_recv[c, j - 1, piece_rows, :].astype(f32)
            scale = rms[p * L : (p + 1) * L, :]
            own_x = x_buf[me, p * L : (p + 1) * L, :].astype(f32)
            value = (
                tok_grad[p : p + 1, own]
                + scale * own_gain * summed
                - own_x * (scale * scale * inner_col[:, p : p + 1])
            )
            staged[c, piece_rows, :] = jnp.where(mask_col[:, p : p + 1] > 0.0, value, 0.0).astype(bf16)
        pltpu.make_async_copy(staged.at[c], grad_out.at[chunk_rows(c)], out_sem.at[c]).start()

    for c in range(chunks):
        pltpu.make_async_copy(staged.at[c], grad_out.at[chunk_rows(c)], out_sem.at[c]).wait()
    for c in range(chunks + 1):
        near_copy(c).wait_send()
        for j in range(1, far):
            far_copy(j, c).wait_send()
            relay_copy(j, c).wait_send()
    for k in range(1, mp):
        branch_copy(k).wait_send()
        inner_copy(k).wait_send()
    for k in range(1, dp):
        every_copy(k).wait_send()
        term_copy(k).wait_send()
    for c in range(chunks):
        near_part(0, c).wait_send()
        for j in range(1, far):
            near_part(j, c).wait_send()
            far_part(j, c).wait_send()


def per_device(
    hidden_in, token_ids, passage_counts, positive_doc, queries, norm_gain, w_gate, w_up, w_down
):
    dp = lax.axis_size("dp")
    mp = lax.axis_size("mp")
    rows, width = hidden_in.shape
    model, hid = w_gate.shape
    query_rows = queries.shape[0]
    passes = rows // L
    most = passes // passage_counts.shape[0]
    chunks = passes // chunk_pass
    crow = chunk_pass * L
    far = mp // 2
    dims = (dp, mp, far, rows, width, model, hid, passes, most, chunks, crow)
    hbm = pl.BlockSpec(memory_space=pl.ANY)
    vmem = pl.BlockSpec(memory_space=pltpu.VMEM)
    dma = pltpu.SemaphoreType.DMA
    wide = model + lane
    few = max(far - 1, 1)
    loss, grad = pl.pallas_call(
        functools.partial(kernel, dims),
        out_shape=(
            jax.ShapeDtypeStruct((1, query_rows), f32),
            jax.ShapeDtypeStruct((rows, width), bf16),
        ),
        in_specs=[hbm] * 5 + [vmem, pl.BlockSpec(memory_space=pltpu.SMEM), vmem, vmem],
        out_specs=(vmem, hbm),
        scratch_shapes=[
            pltpu.VMEM((mp, rows, width), bf16),
            pltpu.VMEM((mp, query_rows, width), bf16),
            pltpu.VMEM((model, hid), bf16),
            pltpu.VMEM((model, hid), bf16),
            pltpu.VMEM((hid, model), bf16),
            pltpu.VMEM((rows, hid), bf16),
            pltpu.VMEM((rows, hid), bf16),
            pltpu.VMEM((rows, hid), bf16),
            pltpu.VMEM((crow, model), bf16),
            pltpu.VMEM((8, lane), bf16),
            pltpu.VMEM((crow, hid), bf16),
            pltpu.VMEM((crow, hid), bf16),
            pltpu.VMEM((rows, 1), f32),
            pltpu.VMEM((2 * passes, hid), f32),
            pltpu.VMEM((2 * passes, model), f32),
            pltpu.VMEM((mp, passes, model), bf16),
            pltpu.VMEM((dp, passes, wide), bf16),
            pltpu.VMEM((dp, passes, wide), bf16),
            pltpu.VMEM((dp, passes, wide), bf16),
            pltpu.VMEM((passes, model), f32),
            pltpu.VMEM((2 * passes, hid), f32),
            pltpu.VMEM((mp, passes, L), f32),
            pltpu.VMEM((passes, L), f32),
            pltpu.VMEM((chunks, far, crow, width), bf16),
            pltpu.VMEM((chunks, far, crow, width), bf16),
            pltpu.VMEM((chunks, few, crow, width), bf16),
            pltpu.VMEM((chunks, few, crow, width), bf16),
            pltpu.VMEM((chunks, crow, width), f32),
            pltpu.VMEM((chunks, crow, width), bf16),
            dma((5,)),
            dma((chunks,)),
            dma((chunks + 1,)),
            dma((chunks + 1,)),
            dma((few, chunks + 1)),
            dma((few, chunks + 1)),
            dma((few, chunks + 1)),
            dma((few, chunks + 1)),
            dma((mp - 1,)),
            dma((mp - 1,)),
            dma((mp - 1,)),
            dma((mp - 1,)),
            dma((dp - 1,)),
            dma((dp - 1,)),
            dma((dp - 1,)),
            dma((dp - 1,)),
            dma((chunks, far)),
            dma((chunks, far)),
            dma((chunks, few)),
            dma((chunks, few)),
        ],
        compiler_params=pltpu.CompilerParams(
            collective_id=0, has_side_effects=True, vmem_limit_bytes=67000000
        ),
        name="gradcache_step",
    )(
        hidden_in,
        queries,
        w_gate,
        w_up,
        w_down,
        token_ids.reshape(passes, L),
        passage_counts,
        positive_doc.reshape(1, query_rows),
        norm_gain.reshape(1, model),
    )
    return loss.reshape(query_rows), grad


def solution(mesh):
    return jax.shard_map(
        per_device,
        mesh=mesh,
        in_specs=(
            P("dp", "mp"),
            P("dp"),
            P("dp"),
            P("dp"),
            P("dp", "mp"),
            P(),
            P(None, "mp"),
            P(None, "mp"),
            P("mp", None),
        ),
        out_specs=(P("dp"), P("dp", "mp")),
        check_vma=False,
    )
```

```python
import functools

import jax
import jax.numpy as jnp
from jax import lax
from jax.experimental import pallas as pl
from jax.experimental.pallas import tpu as pltpu
from jax.sharding import PartitionSpec as P

L = 128

pad_token = 128001
score_scale = 20.0
loss_seed = 4096.0
norm_epsilon = 1e-05
unit_epsilon = 1e-06
lane = 128
chunk_pass = 2
MESH = pl.DeviceIdType.MESH
f32 = jnp.float32
bf16 = jnp.bfloat16


def dot_nn(left, right):
    return lax.dot_general(left, right, (((1,), (0,)), ((), ())), preferred_element_type=f32)


def dot_nt(left, right):
    return lax.dot_general(left, right, (((1,), (1,)), ((), ())), preferred_element_type=f32)


def tile_of(width):
    return 256 if width % 256 == 0 else lane


def kernel(
    dims,
    hidden, queries, w_gate, w_up, w_down, tokens, counts, positive, gain,
    loss_out, grad_out,
    x_buf, q_all, pos_all, wg, wu, wd, a_buf, b_buf, c_buf, normed, dgate, dup, rms,
    act_pool, row_pool, branch_send, branch, square_x, raw_x, mass_x, mass_all, tok_x, tok_grad,
    g_row, inner_x,
    mask_row, near_send, near_recv, far_send, far_recv, kept, staged, sum_gate, sum_up,
    load_sem, out_sem, xn_s, xn_r, xf_s, xf_r, xr_s, xr_r, br_s, br_r, in_s, in_r,
    qu_s, qu_r, po_s, po_r, sq_s, sq_r, ra_s, ra_r, ma_s, ma_r, tk_s, tk_r,
    ns_s, ns_r, fs_s, fs_r,
):
    dp, mp, far, rows, width, model, hid, passes, most, chunks, crow, asked = dims
    asked_all = dp * asked
    me = lax.axis_index("mp")
    dme = lax.axis_index("dp")
    chip, core = me // 2, me % 2
    partner = chip * 2 + (1 - core)

    def same(j):
        return ((chip + j + far) % far) * 2 + core

    def other(j):
        return ((chip + j + far) % far) * 2 + (1 - core)

    def chunk_rows(c):
        return pl.ds(pl.multiple_of(c * crow, crow), crow)

    def remote(src, dst, send, recv, d, m):
        return pltpu.make_async_remote_copy(
            src_ref=src, dst_ref=dst, send_sem=send, recv_sem=recv,
            device_id=(d, m), device_id_type=MESH,
        )

    load_x = pltpu.make_async_copy(hidden, x_buf.at[me], load_sem.at[0])
    load_g = pltpu.make_async_copy(w_gate, wg, load_sem.at[1])
    load_u = pltpu.make_async_copy(w_up, wu, load_sem.at[2])
    load_d = pltpu.make_async_copy(w_down, wd, load_sem.at[3])
    load_q = pltpu.make_async_copy(queries, q_all.at[dme], load_sem.at[4])

    barrier = pltpu.get_barrier_semaphore()
    for k in range(1, mp):
        pl.semaphore_signal(barrier, inc=1, device_id=(dme, (me + k) % mp), device_id_type=MESH)
    for k in range(1, dp):
        pl.semaphore_signal(barrier, inc=1, device_id=((dme + k) % dp, me), device_id_type=MESH)
    load_x.start()
    load_g.start()
    load_u.start()
    load_q.start()
    load_d.start()
    pl.semaphore_wait(barrier, mp - 1 + dp - 1)

    def far_copy(j, c):
        return remote(
            hidden.at[chunk_rows(c)], x_buf.at[me, chunk_rows(c)],
            xf_s.at[j - 1, c], xf_r.at[j - 1, c], dme, same(j),
        )

    def near_copy(c):
        return remote(
            hidden.at[chunk_rows(c)], x_buf.at[me, chunk_rows(c)], xn_s.at[c], xn_r.at[c], dme, partner
        )

    def relay_copy(j, c):
        passed = x_buf.at[same(-j), chunk_rows(c)]
        return remote(passed, passed, xr_s.at[j - 1, c], xr_r.at[j - 1, c], dme, partner)

    def relay(c):
        for j in range(1, far):
            far_copy(j, c).wait_recv()
            relay_copy(j, c).start()

    def query_copy(k):
        return remote(
            queries, q_all.at[dme], qu_s.at[k - 1], qu_r.at[k - 1], (dme + k) % dp, me
        )

    def positive_copy(k):
        return remote(
            positive, pos_all.at[dme], po_s.at[k - 1], po_r.at[k - 1], (dme + k) % dp, me
        )

    for c in range(chunks):
        for j in range(1, far):
            far_copy(j, c).start()
        near_copy(c).start()
    for k in range(1, dp):
        query_copy(k).start()
        positive_copy(k).start()
    pos_all[dme] = positive[...]

    pass_index = lax.broadcasted_iota(jnp.int32, (passes, L), 0)
    count = jnp.zeros((passes, L), jnp.int32)
    for d in range(passes // most):
        count = jnp.where(pass_index // most == d, counts[d], count)
    live = (pass_index % most < count).astype(f32)
    mask = jnp.where(tokens[...] != pad_token, live, 0.0)
    mask_row[...] = mask
    divisor = jnp.maximum(jnp.sum(mask, axis=1, keepdims=True), 1.0)
    act_pool[...] = jnp.zeros_like(act_pool)
    row_pool[...] = jnp.zeros_like(row_pool)
    pool_index = lax.broadcasted_iota(jnp.int32, (2 * passes, L), 0)

    tile = tile_of(hid)
    tiles = hid // tile
    last = chunks - 1
    pair = 2 * width

    def select_of(c):
        return jnp.concatenate(
            [
                jnp.where(pool_index == c * chunk_pass + i, mask_row[pl.ds(c * chunk_pass + i, 1), :], 0.0)
                for i in range(chunk_pass)
            ],
            axis=1,
        ).astype(bf16)

    def scale_of(at):
        squares = jnp.zeros((crow, 1), f32)
        for m in range(mp):
            piece_x = x_buf[m, at, :].astype(f32)
            squares = squares + jnp.sum(piece_x * piece_x, axis=1, keepdims=True)
        scale = lax.rsqrt(squares / model + norm_epsilon)
        rms[at, :] = scale
        return scale

    def activate(gate, up, at, cols, select):
        sig = jax.nn.sigmoid(gate)
        b = gate * sig
        a = up * sig * (1.0 + gate * (1.0 - sig))
        hidden_act = (b * up).astype(bf16)
        a_buf[at, cols] = a.astype(bf16)
        b_buf[at, cols] = b.astype(bf16)
        c_buf[at, cols] = (a * gate + b * up).astype(bf16)
        act_pool[:, cols] += dot_nn(select, hidden_act)

    last_rows = slice(last * crow, chunks * crow)

    def gained(m):
        block_gain = gain[:, pl.ds(pl.multiple_of(m * width, width), width)]
        return (x_buf[m, last_rows, :].astype(f32) * block_gain).astype(bf16)

    def block_rows(m, count=1):
        return pl.ds(pl.multiple_of(m * width, width), count * width)

    load_x.wait()
    near_copy(last).wait_recv()
    for i in range(2):
        normed[:, i * width : (i + 1) * width] = gained(chip * 2 + i)
    load_g.wait()
    load_u.wait()
    for t in range(tiles):
        cols = slice(t * tile, (t + 1) * tile)
        if t == tiles // 2:
            relay(0)
        lead = normed[:, 0:pair]
        sum_gate[:, cols] = dot_nn(lead, wg[block_rows(chip * 2, 2), cols])
        sum_up[:, cols] = dot_nn(lead, wu[block_rows(chip * 2, 2), cols])

    def forward(c, carry):
        at = chunk_rows(c)
        near_copy(c).wait_recv()
        for j in range(1, far):
            relay_copy(j, c).wait_recv()
        select = select_of(c)
        scale = scale_of(at)
        for m in range(mp):
            cols = slice(m * width, (m + 1) * width)
            raw_x = x_buf[m, at, :]
            normed[:, cols] = (raw_x.astype(f32) * scale * gain[:, cols]).astype(bf16)
            row_pool[:, cols] += dot_nn(select, raw_x)
        for t in range(tiles):
            cols = slice(t * tile, (t + 1) * tile)
            gate = dot_nn(normed[...], wg[:, cols])
            up = dot_nn(normed[...], wu[:, cols])
            activate(gate, up, at, cols, select)
            if t == max(tiles - 2, 0):
                @pl.when(c + 1 < last)
                def _():
                    relay(c + 1)
        return carry

    lax.fori_loop(0, last, forward, 0)
    relay(last)
    for j in range(1, far):
        normed[:, (j - 1) * width : j * width] = gained(same(-j))
    for t in range(tiles):
        cols = slice(t * tile, (t + 1) * tile)
        for j in range(1, far):
            lead = normed[:, (j - 1) * width : j * width]
            sum_gate[:, cols] += dot_nn(lead, wg[block_rows(same(-j)), cols])
            sum_up[:, cols] += dot_nn(lead, wu[block_rows(same(-j)), cols])
    for j in range(1, far):
        relay_copy(j, last).wait_recv()
    for j in range(1, far):
        normed[:, (j - 1) * width : j * width] = gained(other(-j))
    last_scale = scale_of(last_rows)
    select = select_of(last)
    for t in range(tiles):
        cols = slice(t * tile, (t + 1) * tile)
        gate = sum_gate[:, cols]
        up = sum_up[:, cols]
        for j in range(1, far):
            lead = normed[:, (j - 1) * width : j * width]
            gate = gate + dot_nn(lead, wg[block_rows(other(-j)), cols])
            up = up + dot_nn(lead, wu[block_rows(other(-j)), cols])
        activate(gate * last_scale, up * last_scale, last_rows, cols, select)
    for m in range(mp):
        cols = slice(m * width, (m + 1) * width)
        row_pool[:, cols] += dot_nn(select, x_buf[m, last_rows, :])

    load_d.wait()
    pooled = act_pool[0:passes, :]
    high = pooled.astype(bf16).astype(f32)
    both = jnp.concatenate([high, pooled - high], axis=0).astype(bf16)
    def to_peer(ref, dst, send, recv, k):
        return remote(ref, dst, send.at[k - 1], recv.at[k - 1], dme, (me + k) % mp)

    def block_lanes(m):
        return pl.ds(pl.multiple_of(m * width, width), width)

    def branch_copy(k):
        return to_peer(branch_send.at[k], branch.at[me], br_s, br_r, k)

    for k in range(1, mp):
        part = dot_nn(both, wd[:, block_lanes((me + k) % mp)])
        branch_send[k] = (part[0:passes] + part[passes:]).astype(bf16)
        branch_copy(k).start()
    part = dot_nn(both, wd[:, block_lanes(me)])
    branch[me] = (part[0:passes] + part[passes:]).astype(bf16)

    load_q.wait()
    for k in range(1, dp):
        query_copy(k).wait_recv()
    ones = jnp.ones((2 * passes, width), bf16)
    for d in range(dp):
        query = q_all[d].astype(f32)
        square = query * query
        top = square.astype(bf16)
        rest = (square - top.astype(f32)).astype(bf16)
        square_x[me, :, d * asked : (d + 1) * asked] = (dot_nt(ones, top) + dot_nt(ones, rest))[0:1, :]

    def square_copy(k):
        return to_peer(square_x.at[me], square_x.at[me], sq_s, sq_r, k)

    for k in range(1, mp):
        square_copy(k).start()

    for k in range(1, mp):
        branch_copy(k).wait_recv()
    own = block_lanes(me)
    total = row_pool[0:passes, own]
    for m in range(mp):
        total = total + branch[m].astype(f32)
    vec = (total / divisor).astype(bf16).astype(f32)
    vec_half = jnp.concatenate([vec, jnp.zeros_like(vec)], axis=0).astype(bf16)
    for d in range(dp):
        raw_x[me, :, d * asked : (d + 1) * asked] = dot_nt(vec_half, q_all[d])[0:passes]
    raw_x[me, :, asked_all:] = jnp.broadcast_to(
        jnp.sum(vec * vec, axis=1, keepdims=True), (passes, lane)
    )

    def raw_copy(k):
        return to_peer(raw_x.at[me], raw_x.at[me], ra_s, ra_r, k)

    for k in range(1, mp):
        raw_copy(k).start()
    for k in range(1, dp):
        positive_copy(k).wait_recv()
    asked_for = jnp.concatenate([pos_all[d] for d in range(dp)], axis=1)
    doc_index = dme * (passes // most) + lax.broadcasted_iota(jnp.int32, (passes, asked_all), 0) // most
    hit = (doc_index == asked_for).astype(f32)
    for k in range(1, mp):
        square_copy(k).wait_recv()
    query_square = square_x[0]
    for m in range(1, mp):
        query_square = query_square + square_x[m]
    query_scale = lax.rsqrt(query_square + unit_epsilon)
    for k in range(1, mp):
        raw_copy(k).wait_recv()

    summed = raw_x[0]
    for m in range(1, mp):
        summed = summed + raw_x[m]
    raw = summed[:, 0:asked_all]
    pass_scale = lax.rsqrt(summed[:, asked_all : asked_all + 1] + unit_epsilon)
    weights = live[:, 0:1] * jnp.exp(score_scale * raw * query_scale * pass_scale)
    mass_x[dme] = jnp.concatenate(
        [jnp.sum(weights, axis=0, keepdims=True), jnp.sum(weights * hit, axis=0, keepdims=True)], axis=0
    )

    def mass_copy(k):
        return remote(
            mass_x.at[dme], mass_x.at[dme], ma_s.at[k - 1], ma_r.at[k - 1], (dme + k) % dp, me
        )

    for k in range(1, dp):
        mass_copy(k).start()
    for k in range(1, dp):
        mass_copy(k).wait_recv()
    masses = mass_x[0]
    for d in range(1, dp):
        masses = masses + mass_x[d]
    mass_all[...] = masses
    mass = masses[0:1, :]
    hit_mass = masses[1:2, :]
    coef = loss_seed * score_scale * query_scale * (weights / mass - hit * weights / hit_mass)
    norm_term = jnp.sum(coef * raw, axis=1, keepdims=True)
    coef_half = jnp.concatenate([coef, jnp.zeros_like(coef)], axis=0).astype(bf16)
    weighted = jnp.zeros((2 * passes, width), f32)
    for d in range(dp):
        weighted = weighted + dot_nn(coef_half[:, d * asked : (d + 1) * asked], q_all[d])
    change = pass_scale * weighted[0:passes] - vec * (
        pass_scale * pass_scale * pass_scale * norm_term
    )
    token = (change / divisor).astype(bf16)
    tok_grad[...] = token.astype(f32)
    tok_x[me] = token

    def token_copy(k):
        return to_peer(tok_x.at[me], tok_x.at[me], tk_s, tk_r, k)

    for k in range(1, mp):
        token_copy(k).start()
    own_asked = pl.ds(pl.multiple_of(dme * asked, asked), asked)
    loss_out[...] = jnp.log(mass_all[0:1, own_asked]) - jnp.log(mass_all[1:2, own_asked])
    for k in range(1, mp):
        token_copy(k).wait_recv()
    token = jnp.concatenate([tok_x[m].astype(f32) for m in range(mp)], axis=1)
    token_half = jnp.concatenate([token, jnp.zeros_like(token)], axis=0).astype(bf16)
    for t in range(hid // tile):
        cols = slice(t * tile, (t + 1) * tile)
        g_row[:, cols] = dot_nt(token_half, wd[cols, :])

    def near_part(j, c):
        return remote(
            near_send.at[c, j], near_recv.at[c, j], ns_s.at[c, j], ns_r.at[c, j], dme, partner
        )

    def far_part(j, c):
        return remote(
            far_send.at[c, j - 1], far_recv.at[c, j - 1], fs_s.at[c, j - 1], fs_r.at[c, j - 1], dme, same(j)
        )

    def backward(c, carry):
        at = chunk_rows(c)
        for i in range(chunk_pass):
            row = g_row[pl.ds(c * chunk_pass + i, 1), :]
            spread = jnp.broadcast_to(row, (L, hid)).astype(bf16)
            here = pl.ds(pl.multiple_of(c * crow + i * L, L), L)
            dgate[i * L : (i + 1) * L, :] = a_buf[here, :] * spread
            dup[i * L : (i + 1) * L, :] = b_buf[here, :] * spread

        def partial(block):
            at_rows = pl.ds(pl.multiple_of(block * width, width), width)
            return dot_nt(dgate[...], wg[at_rows, :]) + dot_nt(dup[...], wu[at_rows, :])

        for j in range(1, far):
            near_send[c, j] = partial(other(j)).astype(bf16)
            near_part(j, c).start()
        for j in range(1, far):
            mine = partial(same(j))
            near_part(j, c).wait_recv()
            far_send[c, j - 1] = (mine + near_recv[c, j].astype(f32)).astype(bf16)
            far_part(j, c).start()
        near_send[c, 0] = partial(other(0)).astype(bf16)
        near_part(0, c).start()
        kept[c] = partial(me)
        return carry

    backward(0, 0)

    g_half = g_row[...].astype(bf16)
    diagonal = jnp.zeros((2 * passes, L), f32)
    for c in range(chunks):
        found = dot_nt(g_half, c_buf[c * crow : (c + 1) * crow, :])
        for i in range(chunk_pass):
            diagonal = diagonal + jnp.where(
                pool_index == c * chunk_pass + i, found[:, i * L : (i + 1) * L], 0.0
            )
    inner_x[me] = diagonal[0:passes]

    def inner_copy(k):
        return remote(
            inner_x.at[me], inner_x.at[me], in_s.at[k - 1], in_r.at[k - 1], dme, (me + k) % mp
        )

    for k in range(1, mp):
        inner_copy(k).start()
    lax.fori_loop(1, chunks, backward, 0)

    for k in range(1, mp):
        inner_copy(k).wait_recv()
    inner = inner_x[0]
    for m in range(1, mp):
        inner = inner + inner_x[m]
    inner_col = jnp.transpose(inner / model)
    mask_col = jnp.transpose(mask_row[...])
    own_gain = gain[:, own]
    for c in range(chunks):
        near_part(0, c).wait_recv()
        for j in range(1, far):
            far_part(j, c).wait_recv()
        for i in range(chunk_pass):
            p = c * chunk_pass + i
            piece_rows = slice(i * L, (i + 1) * L)
            summed = kept[c, piece_rows, :] + near_recv[c, 0, piece_rows, :].astype(f32)
            for j in range(1, far):
                summed = summed + far_recv[c, j - 1, piece_rows, :].astype(f32)
            scale = rms[p * L : (p + 1) * L, :]
            own_x = x_buf[me, p * L : (p + 1) * L, :].astype(f32)
            value = (
                tok_grad[p : p + 1, :]
                + scale * own_gain * summed
                - own_x * (scale * scale * inner_col[:, p : p + 1])
            )
            staged[c, piece_rows, :] = jnp.where(mask_col[:, p : p + 1] > 0.0, value, 0.0).astype(bf16)
        pltpu.make_async_copy(staged.at[c], grad_out.at[chunk_rows(c)], out_sem.at[c]).start()

    for c in range(chunks):
        pltpu.make_async_copy(staged.at[c], grad_out.at[chunk_rows(c)], out_sem.at[c]).wait()
    for c in range(chunks):
        near_copy(c).wait_send()
        for j in range(1, far):
            far_copy(j, c).wait_send()
            relay_copy(j, c).wait_send()
    for k in range(1, mp):
        branch_copy(k).wait_send()
        square_copy(k).wait_send()
        raw_copy(k).wait_send()
        token_copy(k).wait_send()
        inner_copy(k).wait_send()
    for k in range(1, dp):
        query_copy(k).wait_send()
        positive_copy(k).wait_send()
        mass_copy(k).wait_send()
    for c in range(chunks):
        near_part(0, c).wait_send()
        for j in range(1, far):
            near_part(j, c).wait_send()
            far_part(j, c).wait_send()


def per_device(
    hidden_in, token_ids, passage_counts, positive_doc, queries, norm_gain, w_gate, w_up, w_down
):
    dp = lax.axis_size("dp")
    mp = lax.axis_size("mp")
    rows, width = hidden_in.shape
    model, hid = w_gate.shape
    query_rows = queries.shape[0]
    passes = rows // L
    most = passes // passage_counts.shape[0]
    chunks = passes // chunk_pass
    crow = chunk_pass * L
    far = mp // 2
    dims = (dp, mp, far, rows, width, model, hid, passes, most, chunks, crow, query_rows)
    hbm = pl.BlockSpec(memory_space=pl.ANY)
    vmem = pl.BlockSpec(memory_space=pltpu.VMEM)
    dma = pltpu.SemaphoreType.DMA
    few = max(far - 1, 1)
    loss, grad = pl.pallas_call(
        functools.partial(kernel, dims),
        out_shape=(
            jax.ShapeDtypeStruct((1, query_rows), f32),
            jax.ShapeDtypeStruct((rows, width), bf16),
        ),
        in_specs=[hbm] * 5 + [vmem, pl.BlockSpec(memory_space=pltpu.SMEM), vmem, vmem],
        out_specs=(vmem, hbm),
        scratch_shapes=[
            pltpu.VMEM((mp, rows, width), bf16),
            pltpu.VMEM((dp, query_rows, width), bf16),
            pltpu.VMEM((dp, 1, query_rows), jnp.int32),
            pltpu.VMEM((model, hid), bf16),
            pltpu.VMEM((model, hid), bf16),
            pltpu.VMEM((hid, model), bf16),
            pltpu.VMEM((rows, hid), bf16),
            pltpu.VMEM((rows, hid), bf16),
            pltpu.VMEM((rows, hid), bf16),
            pltpu.VMEM((crow, model), bf16),
            pltpu.VMEM((crow, hid), bf16),
            pltpu.VMEM((crow, hid), bf16),
            pltpu.VMEM((rows, 1), f32),
            pltpu.VMEM((2 * passes, hid), f32),
            pltpu.VMEM((2 * passes, model), f32),
            pltpu.VMEM((mp, passes, width), bf16),
            pltpu.VMEM((mp, passes, width), bf16),
            pltpu.VMEM((mp, 1, dp * query_rows), f32),
            pltpu.VMEM((mp, passes, dp * query_rows + lane), f32),
            pltpu.VMEM((dp, 2, dp * query_rows), f32),
            pltpu.VMEM((2, dp * query_rows), f32),
            pltpu.VMEM((mp, passes, width), bf16),
            pltpu.VMEM((passes, width), f32),
            pltpu.VMEM((2 * passes, hid), f32),
            pltpu.VMEM((mp, passes, L), f32),
            pltpu.VMEM((passes, L), f32),
            pltpu.VMEM((chunks, far, crow, width), bf16),
            pltpu.VMEM((chunks, far, crow, width), bf16),
            pltpu.VMEM((chunks, few, crow, width), bf16),
            pltpu.VMEM((chunks, few, crow, width), bf16),
            pltpu.VMEM((chunks, crow, width), f32),
            pltpu.VMEM((chunks, crow, width), bf16),
            pltpu.VMEM((crow, hid), f32),
            pltpu.VMEM((crow, hid), f32),
            dma((5,)),
            dma((chunks,)),
            dma((chunks,)),
            dma((chunks,)),
            dma((few, chunks)),
            dma((few, chunks)),
            dma((few, chunks)),
            dma((few, chunks)),
            dma((mp - 1,)),
            dma((mp - 1,)),
            dma((mp - 1,)),
            dma((mp - 1,)),
            dma((dp - 1,)),
            dma((dp - 1,)),
            dma((dp - 1,)),
            dma((dp - 1,)),
            dma((mp - 1,)),
            dma((mp - 1,)),
            dma((mp - 1,)),
            dma((mp - 1,)),
            dma((dp - 1,)),
            dma((dp - 1,)),
            dma((mp - 1,)),
            dma((mp - 1,)),
            dma((chunks, far)),
            dma((chunks, far)),
            dma((chunks, few)),
            dma((chunks, few)),
        ],
        compiler_params=pltpu.CompilerParams(
            collective_id=0, has_side_effects=True, vmem_limit_bytes=67000000
        ),
        name="gradcache_step",
    )(
        hidden_in,
        queries,
        w_gate,
        w_up,
        w_down,
        token_ids.reshape(passes, L),
        passage_counts,
        positive_doc.reshape(1, query_rows),
        norm_gain.reshape(1, model),
    )
    def hand_on(loss_in, grad_in, loss_to, grad_to):
        loss_to[...] = loss_in[0, :]
        grad_to[...] = grad_in[...]

    return tuple(
        pl.pallas_call(
            hand_on,
            grid=(2,),
            out_shape=(
                jax.ShapeDtypeStruct((query_rows,), f32),
                jax.ShapeDtypeStruct((rows, width), bf16),
            ),
            in_specs=[
                pl.BlockSpec((1, query_rows), lambda i: (0, 0)),
                pl.BlockSpec((rows // 2, width), lambda i: (i, 0)),
            ],
            out_specs=(
                pl.BlockSpec((query_rows,), lambda i: (0,)),
                pl.BlockSpec((rows // 2, width), lambda i: (i, 0)),
            ),
            name="hand_on",
        )(loss, grad)
    )


def solution(mesh):
    return jax.shard_map(
        per_device,
        mesh=mesh,
        in_specs=(
            P("dp", "mp"),
            P("dp"),
            P("dp"),
            P("dp"),
            P("dp", "mp"),
            P(),
            P(None, "mp"),
            P(None, "mp"),
            P("mp", None),
        ),
        out_specs=(P("dp"), P("dp", "mp")),
        check_vma=False,
    )
```

```python
import functools

import jax
import jax.numpy as jnp
from jax import lax
from jax.experimental import pallas as pl
from jax.experimental.pallas import tpu as pltpu
from jax.sharding import PartitionSpec as P

L = 128

pad_token = 128001
score_scale = 20.0
loss_seed = 4096.0
norm_epsilon = 1e-05
unit_epsilon = 1e-06
lane = 128
chunk_pass = 2
MESH = pl.DeviceIdType.MESH
f32 = jnp.float32
bf16 = jnp.bfloat16


def dot_nn(left, right):
    return lax.dot_general(left, right, (((1,), (0,)), ((), ())), preferred_element_type=f32)


def dot_nt(left, right):
    return lax.dot_general(left, right, (((1,), (1,)), ((), ())), preferred_element_type=f32)


def tile_of(width):
    return 256 if width % 256 == 0 else lane


def kernel(
    dims,
    hidden, queries, w_gate, w_up, w_down, tokens, counts, positive, gain,
    loss_out, grad_out,
    x_buf, q_all, pos_all, wg, wu, wd, a_buf, b_buf, c_buf, normed, dgate, dup, rms,
    act_pool, row_pool, branch_send, branch, square_x, raw_x, mass_x, mass_all, tok_x, tok_grad,
    g_row, inner_x,
    mask_row, near_send, near_recv, far_send, far_recv, kept, staged, sum_gate, sum_up,
    load_sem, out_sem, xn_s, xn_r, xf_s, xf_r, xr_s, xr_r, br_s, br_r, in_s, in_r,
    qu_s, qu_r, po_s, po_r, sq_s, sq_r, ra_s, ra_r, ma_s, ma_r, tk_s, tk_r,
    ns_s, ns_r, fs_s, fs_r,
):
    dp, mp, far, rows, width, model, hid, passes, most, chunks, crow, asked = dims
    asked_all = dp * asked
    me = lax.axis_index("mp")
    dme = lax.axis_index("dp")
    chip, core = me // 2, me % 2
    partner = chip * 2 + (1 - core)

    def same(j):
        return ((chip + j + far) % far) * 2 + core

    def other(j):
        return ((chip + j + far) % far) * 2 + (1 - core)

    def chunk_rows(c):
        return pl.ds(pl.multiple_of(c * crow, crow), crow)

    def remote(src, dst, send, recv, d, m):
        return pltpu.make_async_remote_copy(
            src_ref=src, dst_ref=dst, send_sem=send, recv_sem=recv,
            device_id=(d, m), device_id_type=MESH,
        )

    load_x = pltpu.make_async_copy(hidden, x_buf.at[me], load_sem.at[0])
    load_g = pltpu.make_async_copy(w_gate, wg, load_sem.at[1])
    load_u = pltpu.make_async_copy(w_up, wu, load_sem.at[2])
    load_d = pltpu.make_async_copy(w_down, wd, load_sem.at[3])
    load_q = pltpu.make_async_copy(queries, q_all.at[dme], load_sem.at[4])

    barrier = pltpu.get_barrier_semaphore()
    for k in range(1, mp):
        pl.semaphore_signal(barrier, inc=1, device_id=(dme, (me + k) % mp), device_id_type=MESH)
    for k in range(1, dp):
        pl.semaphore_signal(barrier, inc=1, device_id=((dme + k) % dp, me), device_id_type=MESH)
    load_x.start()
    load_g.start()
    load_u.start()
    load_q.start()
    load_d.start()
    pl.semaphore_wait(barrier, mp - 1 + dp - 1)

    def far_copy(j, c):
        return remote(
            hidden.at[chunk_rows(c)], x_buf.at[me, chunk_rows(c)],
            xf_s.at[j - 1, c], xf_r.at[j - 1, c], dme, same(j),
        )

    def near_copy(c):
        return remote(
            hidden.at[chunk_rows(c)], x_buf.at[me, chunk_rows(c)], xn_s.at[c], xn_r.at[c], dme, partner
        )

    def relay_copy(j, c):
        passed = x_buf.at[same(-j), chunk_rows(c)]
        return remote(passed, passed, xr_s.at[j - 1, c], xr_r.at[j - 1, c], dme, partner)

    def relay(c):
        for j in range(1, far):
            far_copy(j, c).wait_recv()
            relay_copy(j, c).start()

    def query_copy(k):
        return remote(
            queries, q_all.at[dme], qu_s.at[k - 1], qu_r.at[k - 1], (dme + k) % dp, me
        )

    def positive_copy(k):
        return remote(
            positive, pos_all.at[dme], po_s.at[k - 1], po_r.at[k - 1], (dme + k) % dp, me
        )

    for c in range(chunks):
        for j in range(1, far):
            far_copy(j, c).start()
        near_copy(c).start()
    for k in range(1, dp):
        query_copy(k).start()
        positive_copy(k).start()
    pos_all[dme] = positive[...]

    pass_index = lax.broadcasted_iota(jnp.int32, (passes, L), 0)
    count = jnp.zeros((passes, L), jnp.int32)
    for d in range(passes // most):
        count = jnp.where(pass_index // most == d, counts[d], count)
    live = (pass_index % most < count).astype(f32)
    mask = jnp.where(tokens[...] != pad_token, live, 0.0)
    mask_row[...] = mask
    divisor = jnp.maximum(jnp.sum(mask, axis=1, keepdims=True), 1.0)
    act_pool[...] = jnp.zeros_like(act_pool)
    row_pool[...] = jnp.zeros_like(row_pool)
    pool_index = lax.broadcasted_iota(jnp.int32, (2 * passes, L), 0)

    tile = tile_of(hid)
    tiles = hid // tile
    pair = 2 * width

    def select_of(c):
        return jnp.concatenate(
            [
                jnp.where(pool_index == c * chunk_pass + i, mask_row[pl.ds(c * chunk_pass + i, 1), :], 0.0)
                for i in range(chunk_pass)
            ],
            axis=1,
        ).astype(bf16)

    def scale_of(at):
        squares = jnp.zeros((crow, 1), f32)
        for m in range(mp):
            piece_x = x_buf[m, at, :].astype(f32)
            squares = squares + jnp.sum(piece_x * piece_x, axis=1, keepdims=True)
        scale = lax.rsqrt(squares / model + norm_epsilon)
        rms[at, :] = scale
        return scale

    def activate(gate, up, at, cols, select):
        sig = jax.nn.sigmoid(gate)
        b = gate * sig
        a = up * sig * (1.0 + gate * (1.0 - sig))
        hidden_act = (b * up).astype(bf16)
        a_buf[at, cols] = a.astype(bf16)
        b_buf[at, cols] = b.astype(bf16)
        c_buf[at, cols] = (a * gate + b * up).astype(bf16)
        act_pool[:, cols] += dot_nn(select, hidden_act)

    late = max(chunks - 2, 0)

    def gained(m, c):
        block_gain = gain[:, pl.ds(pl.multiple_of(m * width, width), width)]
        return (x_buf[m, c * crow : (c + 1) * crow, :].astype(f32) * block_gain).astype(bf16)

    def block_rows(m, count=1):
        return pl.ds(pl.multiple_of(m * width, width), count * width)

    load_x.wait()
    load_g.wait()
    load_u.wait()
    for c in range(chunks - 1, late - 1, -1):
        near_copy(c).wait_recv()
        for i in range(2):
            normed[:, i * width : (i + 1) * width] = gained(chip * 2 + i, c)
        for t in range(tiles):
            cols = slice(t * tile, (t + 1) * tile)
            if c == late and t == tiles // 2:
                relay(0)
            lead = normed[:, 0:pair]
            sum_gate[c - late, :, cols] = dot_nn(lead, wg[block_rows(chip * 2, 2), cols])
            sum_up[c - late, :, cols] = dot_nn(lead, wu[block_rows(chip * 2, 2), cols])

    def forward(c, carry):
        at = chunk_rows(c)
        near_copy(c).wait_recv()
        for j in range(1, far):
            relay_copy(j, c).wait_recv()
        select = select_of(c)
        scale = scale_of(at)
        for m in range(mp):
            cols = slice(m * width, (m + 1) * width)
            raw_x = x_buf[m, at, :]
            normed[:, cols] = (raw_x.astype(f32) * scale * gain[:, cols]).astype(bf16)
            row_pool[:, cols] += dot_nn(select, raw_x)
        for t in range(tiles):
            cols = slice(t * tile, (t + 1) * tile)
            gate = dot_nn(normed[...], wg[:, cols])
            up = dot_nn(normed[...], wu[:, cols])
            activate(gate, up, at, cols, select)
            if t == tiles // 2 + 1:
                @pl.when(c + 1 < late)
                def _():
                    relay(c + 1)
        return carry

    lax.fori_loop(0, late, forward, 0)
    for c in range(late, chunks):
        at = slice(c * crow, (c + 1) * crow)
        if c > 0:
            relay(c)
        for j in range(1, far):
            normed[:, (j - 1) * width : j * width] = gained(same(-j), c)
        for t in range(tiles):
            cols = slice(t * tile, (t + 1) * tile)
            for j in range(1, far):
                lead = normed[:, (j - 1) * width : j * width]
                sum_gate[c - late, :, cols] += dot_nn(lead, wg[block_rows(same(-j)), cols])
                sum_up[c - late, :, cols] += dot_nn(lead, wu[block_rows(same(-j)), cols])
        for j in range(1, far):
            relay_copy(j, c).wait_recv()
        for j in range(1, far):
            normed[:, (j - 1) * width : j * width] = gained(other(-j), c)
        late_scale = scale_of(at)
        select = select_of(c)
        for t in range(tiles):
            cols = slice(t * tile, (t + 1) * tile)
            gate = sum_gate[c - late, :, cols]
            up = sum_up[c - late, :, cols]
            for j in range(1, far):
                lead = normed[:, (j - 1) * width : j * width]
                gate = gate + dot_nn(lead, wg[block_rows(other(-j)), cols])
                up = up + dot_nn(lead, wu[block_rows(other(-j)), cols])
            activate(gate * late_scale, up * late_scale, at, cols, select)
        for m in range(mp):
            cols = slice(m * width, (m + 1) * width)
            row_pool[:, cols] += dot_nn(select, x_buf[m, at, :])

    load_d.wait()
    pooled = act_pool[0:passes, :]
    high = pooled.astype(bf16).astype(f32)
    both = jnp.concatenate([high, pooled - high], axis=0).astype(bf16)
    def to_peer(ref, dst, send, recv, k):
        return remote(ref, dst, send.at[k - 1], recv.at[k - 1], dme, (me + k) % mp)

    def block_lanes(m):
        return pl.ds(pl.multiple_of(m * width, width), width)

    def branch_copy(k):
        return to_peer(branch_send.at[k], branch.at[me], br_s, br_r, k)

    for k in range(1, mp):
        part = dot_nn(both, wd[:, block_lanes((me + k) % mp)])
        branch_send[k] = (part[0:passes] + part[passes:]).astype(bf16)
        branch_copy(k).start()
    part = dot_nn(both, wd[:, block_lanes(me)])
    branch[me] = (part[0:passes] + part[passes:]).astype(bf16)

    load_q.wait()
    for k in range(1, dp):
        query_copy(k).wait_recv()
    ones = jnp.ones((2 * passes, width), bf16)
    for d in range(dp):
        query = q_all[d].astype(f32)
        square = query * query
        top = square.astype(bf16)
        rest = (square - top.astype(f32)).astype(bf16)
        square_x[me, :, d * asked : (d + 1) * asked] = (dot_nt(ones, top) + dot_nt(ones, rest))[0:1, :]

    def square_copy(k):
        return to_peer(square_x.at[me], square_x.at[me], sq_s, sq_r, k)

    for k in range(1, mp):
        square_copy(k).start()

    for k in range(1, mp):
        branch_copy(k).wait_recv()
    own = block_lanes(me)
    total = row_pool[0:passes, own]
    for m in range(mp):
        total = total + branch[m].astype(f32)
    vec = (total / divisor).astype(bf16).astype(f32)
    vec_half = jnp.concatenate([vec, jnp.zeros_like(vec)], axis=0).astype(bf16)
    for d in range(dp):
        raw_x[me, :, d * asked : (d + 1) * asked] = dot_nt(vec_half, q_all[d])[0:passes]
    raw_x[me, :, asked_all:] = jnp.broadcast_to(
        jnp.sum(vec * vec, axis=1, keepdims=True), (passes, lane)
    )

    def raw_copy(k):
        return to_peer(raw_x.at[me], raw_x.at[me], ra_s, ra_r, k)

    for k in range(1, mp):
        raw_copy(k).start()
    for k in range(1, dp):
        positive_copy(k).wait_recv()
    asked_for = jnp.concatenate([pos_all[d] for d in range(dp)], axis=1)
    doc_index = dme * (passes // most) + lax.broadcasted_iota(jnp.int32, (passes, asked_all), 0) // most
    hit = (doc_index == asked_for).astype(f32)
    for k in range(1, mp):
        square_copy(k).wait_recv()
    query_square = square_x[0]
    for m in range(1, mp):
        query_square = query_square + square_x[m]
    query_scale = lax.rsqrt(query_square + unit_epsilon)
    for k in range(1, mp):
        raw_copy(k).wait_recv()

    summed = raw_x[0]
    for m in range(1, mp):
        summed = summed + raw_x[m]
    raw = summed[:, 0:asked_all]
    pass_scale = lax.rsqrt(summed[:, asked_all : asked_all + 1] + unit_epsilon)
    weights = live[:, 0:1] * jnp.exp(score_scale * raw * query_scale * pass_scale)
    mass_x[dme] = jnp.concatenate(
        [jnp.sum(weights, axis=0, keepdims=True), jnp.sum(weights * hit, axis=0, keepdims=True)], axis=0
    )

    def mass_copy(k):
        return remote(
            mass_x.at[dme], mass_x.at[dme], ma_s.at[k - 1], ma_r.at[k - 1], (dme + k) % dp, me
        )

    for k in range(1, dp):
        mass_copy(k).start()
    for k in range(1, dp):
        mass_copy(k).wait_recv()
    masses = mass_x[0]
    for d in range(1, dp):
        masses = masses + mass_x[d]
    mass_all[...] = masses
    mass = masses[0:1, :]
    hit_mass = masses[1:2, :]
    coef = loss_seed * score_scale * query_scale * (weights / mass - hit * weights / hit_mass)
    norm_term = jnp.sum(coef * raw, axis=1, keepdims=True)
    coef_half = jnp.concatenate([coef, jnp.zeros_like(coef)], axis=0).astype(bf16)
    weighted = jnp.zeros((2 * passes, width), f32)
    for d in range(dp):
        weighted = weighted + dot_nn(coef_half[:, d * asked : (d + 1) * asked], q_all[d])
    change = pass_scale * weighted[0:passes] - vec * (
        pass_scale * pass_scale * pass_scale * norm_term
    )
    token = (change / divisor).astype(bf16)
    tok_grad[...] = token.astype(f32)
    tok_x[me] = token

    def token_copy(k):
        return to_peer(tok_x.at[me], tok_x.at[me], tk_s, tk_r, k)

    for k in range(1, mp):
        token_copy(k).start()
    own_asked = pl.ds(pl.multiple_of(dme * asked, asked), asked)
    loss_out[...] = jnp.log(mass_all[0:1, own_asked]) - jnp.log(mass_all[1:2, own_asked])
    for k in range(1, mp):
        token_copy(k).wait_recv()
    token = jnp.concatenate([tok_x[m].astype(f32) for m in range(mp)], axis=1)
    token_half = jnp.concatenate([token, jnp.zeros_like(token)], axis=0).astype(bf16)
    for t in range(hid // tile):
        cols = slice(t * tile, (t + 1) * tile)
        g_row[:, cols] = dot_nt(token_half, wd[cols, :])

    def near_part(j, c):
        return remote(
            near_send.at[c, j], near_recv.at[c, j], ns_s.at[c, j], ns_r.at[c, j], dme, partner
        )

    def far_part(j, c):
        return remote(
            far_send.at[c, j - 1], far_recv.at[c, j - 1], fs_s.at[c, j - 1], fs_r.at[c, j - 1], dme, same(j)
        )

    def inner_copy(k):
        return remote(
            inner_x.at[me], inner_x.at[me], in_s.at[k - 1], in_r.at[k - 1], dme, (me + k) % mp
        )

    def backward(c, carry):
        at = chunk_rows(c)
        for i in range(chunk_pass):
            row = g_row[pl.ds(c * chunk_pass + i, 1), :]
            spread = jnp.broadcast_to(row, (L, hid)).astype(bf16)
            here = pl.ds(pl.multiple_of(c * crow + i * L, L), L)
            dgate[i * L : (i + 1) * L, :] = a_buf[here, :] * spread
            dup[i * L : (i + 1) * L, :] = b_buf[here, :] * spread

        def partial(block):
            at_rows = pl.ds(pl.multiple_of(block * width, width), width)
            return dot_nt(dgate[...], wg[at_rows, :]) + dot_nt(dup[...], wu[at_rows, :])

        for j in range(1, far):
            near_send[c, j] = partial(other(j)).astype(bf16)
            near_part(j, c).start()
        for j in range(1, far):
            mine = partial(same(j))
            near_part(j, c).wait_recv()
            far_send[c, j - 1] = (mine + near_recv[c, j].astype(f32)).astype(bf16)
            far_part(j, c).start()
        near_send[c, 0] = partial(other(0)).astype(bf16)
        near_part(0, c).start()
        kept[c] = partial(me)

        @pl.when(c == 0)
        def _():
            g_half = g_row[...].astype(bf16)
            diagonal = jnp.zeros((2 * passes, L), f32)
            for c in range(chunks):
                found = dot_nt(g_half, c_buf[c * crow : (c + 1) * crow, :])
                for i in range(chunk_pass):
                    diagonal = diagonal + jnp.where(
                        pool_index == c * chunk_pass + i, found[:, i * L : (i + 1) * L], 0.0
                    )
            inner_x[me] = diagonal[0:passes]
            for k in range(1, mp):
                inner_copy(k).start()

        return carry

    lax.fori_loop(0, chunks, backward, 0)

    for k in range(1, mp):
        inner_copy(k).wait_recv()
    inner = inner_x[0]
    for m in range(1, mp):
        inner = inner + inner_x[m]
    inner_col = jnp.transpose(inner / model)
    mask_col = jnp.transpose(mask_row[...])
    own_gain = gain[:, own]
    for c in range(chunks):
        near_part(0, c).wait_recv()
        for j in range(1, far):
            far_part(j, c).wait_recv()
        for i in range(chunk_pass):
            p = c * chunk_pass + i
            piece_rows = slice(i * L, (i + 1) * L)
            summed = kept[c, piece_rows, :] + near_recv[c, 0, piece_rows, :].astype(f32)
            for j in range(1, far):
                summed = summed + far_recv[c, j - 1, piece_rows, :].astype(f32)
            scale = rms[p * L : (p + 1) * L, :]
            own_x = x_buf[me, p * L : (p + 1) * L, :].astype(f32)
            value = (
                tok_grad[p : p + 1, :]
                + scale * own_gain * summed
                - own_x * (scale * scale * inner_col[:, p : p + 1])
            )
            staged[c, piece_rows, :] = jnp.where(mask_col[:, p : p + 1] > 0.0, value, 0.0).astype(bf16)
        pltpu.make_async_copy(staged.at[c], grad_out.at[chunk_rows(c)], out_sem.at[c]).start()

    for c in range(chunks):
        pltpu.make_async_copy(staged.at[c], grad_out.at[chunk_rows(c)], out_sem.at[c]).wait()
    for c in range(chunks):
        near_copy(c).wait_send()
        for j in range(1, far):
            far_copy(j, c).wait_send()
            relay_copy(j, c).wait_send()
    for k in range(1, mp):
        branch_copy(k).wait_send()
        square_copy(k).wait_send()
        raw_copy(k).wait_send()
        token_copy(k).wait_send()
        inner_copy(k).wait_send()
    for k in range(1, dp):
        query_copy(k).wait_send()
        positive_copy(k).wait_send()
        mass_copy(k).wait_send()
    for c in range(chunks):
        near_part(0, c).wait_send()
        for j in range(1, far):
            near_part(j, c).wait_send()
            far_part(j, c).wait_send()


def per_device(
    hidden_in, token_ids, passage_counts, positive_doc, queries, norm_gain, w_gate, w_up, w_down
):
    dp = lax.axis_size("dp")
    mp = lax.axis_size("mp")
    rows, width = hidden_in.shape
    model, hid = w_gate.shape
    query_rows = queries.shape[0]
    passes = rows // L
    most = passes // passage_counts.shape[0]
    chunks = passes // chunk_pass
    crow = chunk_pass * L
    far = mp // 2
    dims = (dp, mp, far, rows, width, model, hid, passes, most, chunks, crow, query_rows)
    hbm = pl.BlockSpec(memory_space=pl.ANY)
    vmem = pl.BlockSpec(memory_space=pltpu.VMEM)
    dma = pltpu.SemaphoreType.DMA
    few = max(far - 1, 1)
    loss, grad = pl.pallas_call(
        functools.partial(kernel, dims),
        out_shape=(
            jax.ShapeDtypeStruct((1, query_rows), f32),
            jax.ShapeDtypeStruct((rows, width), bf16),
        ),
        in_specs=[hbm] * 5 + [vmem, pl.BlockSpec(memory_space=pltpu.SMEM), vmem, vmem],
        out_specs=(vmem, hbm),
        scratch_shapes=[
            pltpu.VMEM((mp, rows, width), bf16),
            pltpu.VMEM((dp, query_rows, width), bf16),
            pltpu.VMEM((dp, 1, query_rows), jnp.int32),
            pltpu.VMEM((model, hid), bf16),
            pltpu.VMEM((model, hid), bf16),
            pltpu.VMEM((hid, model), bf16),
            pltpu.VMEM((rows, hid), bf16),
            pltpu.VMEM((rows, hid), bf16),
            pltpu.VMEM((rows, hid), bf16),
            pltpu.VMEM((crow, model), bf16),
            pltpu.VMEM((crow, hid), bf16),
            pltpu.VMEM((crow, hid), bf16),
            pltpu.VMEM((rows, 1), f32),
            pltpu.VMEM((2 * passes, hid), f32),
            pltpu.VMEM((2 * passes, model), f32),
            pltpu.VMEM((mp, passes, width), bf16),
            pltpu.VMEM((mp, passes, width), bf16),
            pltpu.VMEM((mp, 1, dp * query_rows), f32),
            pltpu.VMEM((mp, passes, dp * query_rows + lane), f32),
            pltpu.VMEM((dp, 2, dp * query_rows), f32),
            pltpu.VMEM((2, dp * query_rows), f32),
            pltpu.VMEM((mp, passes, width), bf16),
            pltpu.VMEM((passes, width), f32),
            pltpu.VMEM((2 * passes, hid), f32),
            pltpu.VMEM((mp, passes, L), f32),
            pltpu.VMEM((passes, L), f32),
            pltpu.VMEM((chunks, far, crow, width), bf16),
            pltpu.VMEM((chunks, far, crow, width), bf16),
            pltpu.VMEM((chunks, few, crow, width), bf16),
            pltpu.VMEM((chunks, few, crow, width), bf16),
            pltpu.VMEM((chunks, crow, width), f32),
            pltpu.VMEM((chunks, crow, width), bf16),
            pltpu.VMEM((min(chunks, 2), crow, hid), f32),
            pltpu.VMEM((min(chunks, 2), crow, hid), f32),
            dma((5,)),
            dma((chunks,)),
            dma((chunks,)),
            dma((chunks,)),
            dma((few, chunks)),
            dma((few, chunks)),
            dma((few, chunks)),
            dma((few, chunks)),
            dma((mp - 1,)),
            dma((mp - 1,)),
            dma((mp - 1,)),
            dma((mp - 1,)),
            dma((dp - 1,)),
            dma((dp - 1,)),
            dma((dp - 1,)),
            dma((dp - 1,)),
            dma((mp - 1,)),
            dma((mp - 1,)),
            dma((mp - 1,)),
            dma((mp - 1,)),
            dma((dp - 1,)),
            dma((dp - 1,)),
            dma((mp - 1,)),
            dma((mp - 1,)),
            dma((chunks, far)),
            dma((chunks, far)),
            dma((chunks, few)),
            dma((chunks, few)),
        ],
        compiler_params=pltpu.CompilerParams(
            collective_id=0, has_side_effects=True, vmem_limit_bytes=67000000
        ),
        name="gradcache_step",
    )(
        hidden_in,
        queries,
        w_gate,
        w_up,
        w_down,
        token_ids.reshape(passes, L),
        passage_counts,
        positive_doc.reshape(1, query_rows),
        norm_gain.reshape(1, model),
    )
    def hand_on(loss_in, grad_in, loss_to, grad_to):
        loss_to[...] = loss_in[0, :]
        grad_to[...] = grad_in[...]

    return tuple(
        pl.pallas_call(
            hand_on,
            grid=(2,),
            out_shape=(
                jax.ShapeDtypeStruct((query_rows,), f32),
                jax.ShapeDtypeStruct((rows, width), bf16),
            ),
            in_specs=[
                pl.BlockSpec((1, query_rows), lambda i: (0, 0)),
                pl.BlockSpec((rows // 2, width), lambda i: (i, 0)),
            ],
            out_specs=(
                pl.BlockSpec((query_rows,), lambda i: (0,)),
                pl.BlockSpec((rows // 2, width), lambda i: (i, 0)),
            ),
            name="hand_on",
        )(loss, grad)
    )


def solution(mesh):
    return jax.shard_map(
        per_device,
        mesh=mesh,
        in_specs=(
            P("dp", "mp"),
            P("dp"),
            P("dp"),
            P("dp"),
            P("dp", "mp"),
            P(),
            P(None, "mp"),
            P(None, "mp"),
            P("mp", None),
        ),
        out_specs=(P("dp"), P("dp", "mp")),
        check_vma=False,
    )
```
